32 devices in a mesh: sky: 8 (over y, x, core), tm: 4 (over z).
Axes of the slice: x: 2, y: 2, z: 4, core: 2. Of those that a mesh axis runs over, the one named last changes fastest.
Arguments:
- obs_source: int32 [131072], P(('sky', 'tm')), may hold values from 0 to 1023
- obs_knot: int32 [131072], P(('sky', 'tm')), may hold values from 0 to 2047, as said below
- obs_count: int32 [32], P(('sky', 'tm')), may hold values from 256 to 4096, as said below
- src_design: float32 [5, 131072], P(None, ('sky', 'tm')), may hold values from -3 to 3
- att_design: float32 [4, 131072], P(None, ('sky', 'tm')), may hold values from -6 to 6
- obs_phase: float32 [131072], P(('sky', 'tm')), may hold values from 0 to 1
- obs_value: float32 [131072], P(('sky', 'tm')), may hold values from -6 to 6
- src_prior: float32 [5, 8192], P(None, 'sky'), may hold values from 1 to 16
Outputs:
- att_solution: float32 [4, 4, 2048], P(None, 'tm', 'sky')
- att_residual: float32 [4, 4, 2048], P(None, 'tm', 'sky')
- source_solution: float32 [5, 8192], P(None, 'sky')
The draws below stay inside these ranges and needn't reach their ends.
Inputs may be any that keep to these rules, and one draw needn't show every extreme that they name: Block b holds the 4096 observation slots o with o // 4096 = b; with i = b // 4 its sources are the sources i * 1024 + obs_source. With j = b % 4 for the observation's block b, its four spline knots are j * 2048 + obs_knot and the next three. In every block, each range of 256 values r * 256 to r * 256 + 255 of obs_knot holds exactly 512 of the block's slots. `obs_count`: each count is 4096 divided by 1, 2, 4, 8 or 16; the live slots of a block are its first ones; some block is full.
All inputs are finite; a program needn't handle non-finite values.
Results may differ from the reference program's by a relative error of at most 0.0001.
Values sent between devices are 32-bit elements; how exact they have to be, the bound alone decides.
A program may use at most 64 MiB of HBM per device.

```python
import math
import jax
import jax.numpy as jnp
from jax import lax

PARAMS = 5
COMP = 4
ITERS = 2
SRC_DEV = 1024
OBS_DEV = 4096
KN_DEV = 256
KSEG = 2048
KNOTS = 8192
SOURCES = 8192
BLOCKS = 32
OBS = 131072
N_TM = 4


def draw_obs_count(key, part):
    shifts = jax.random.randint(jax.random.fold_in(key, 11), (BLOCKS,), 0, 5)
    fullest = jax.random.randint(jax.random.fold_in(key, 12), (), 0, BLOCKS)
    shifts = jnp.where(jnp.arange(BLOCKS) == fullest, 0, shifts).astype(jnp.int32)
    return jnp.right_shift(jnp.full((BLOCKS,), OBS_DEV, jnp.int32), shifts)


def shuffle(block_key):
    return jax.random.permutation(block_key, OBS_DEV)


def draw_obs_knot(key, part):
    span_count = KSEG // KN_DEV
    block_keys = jax.random.split(jax.random.fold_in(key, 21), BLOCKS)
    orders = jax.vmap(shuffle)(block_keys)
    owners = (orders % span_count).reshape(-1)
    offsets = jax.random.randint(jax.random.fold_in(key, 22), (OBS,), 0, KN_DEV)
    return (owners * KN_DEV + offsets).astype(jnp.int32)


def plant(entries, key, smallest, high):
    spot = [jax.random.randint(jax.random.fold_in(key, axis), (), 0, length) for axis, length in enumerate(entries.shape)]
    widest = entries.shape.index(max(entries.shape))
    neighbour = spot[:widest] + [(spot[widest] + 1) % entries.shape[widest]] + spot[widest + 1:]
    return entries.at[tuple(spot)].set(smallest).at[tuple(neighbour)].set(high)


def shard_levels(own_key, shape, pieces, least, high):
    loudness = 1.0
    for dim, shards_of in pieces:
        heights = jax.random.uniform(jax.random.fold_in(jax.random.fold_in(own_key, 6), dim), (shards_of,), jnp.float32, least / len(pieces), high / len(pieces))
        loudness = loudness * jnp.repeat(jnp.exp(heights), shape[dim] // shards_of).reshape((-1,) + (1,) * (len(shape) - 1 - dim))
    return loudness


def scatter_about(stream_key, shape, width, reach, pieces=(), kind=jnp.bfloat16):
    loudness = shard_levels(stream_key, shape, pieces, -0.22, 0.18) if pieces else 1.0
    values = jax.random.normal(stream_key, shape, jnp.float32) * width * loudness
    return jnp.minimum(jnp.maximum(values, -reach), reach).astype(kind)


def setup_inputs(seed: int = 0) -> dict:
    splits = jax.random.split(jax.random.key(seed), 9)
    return {
        "obs_source": plant(jax.random.randint(splits[0], (OBS,), 0, SRC_DEV), jax.random.fold_in(splits[0], 1), 0, SRC_DEV - 1).astype(jnp.int32),
        "obs_knot": draw_obs_knot(jax.random.fold_in(splits[8], 71), 0),
        "obs_count": draw_obs_count(jax.random.fold_in(splits[8], 71), 0),
        "src_design": scatter_about(splits[3], (PARAMS, OBS), 0.5, 3.0, ((1, 32),), jnp.float32),
        "att_design": scatter_about(splits[4], (COMP, OBS), 1.0, 6.0, ((1, 32),), jnp.float32),
        "obs_phase": jnp.clip(1.0 * jax.random.uniform(splits[5], (OBS,), jnp.float32) ** shard_levels(splits[5], (OBS,), ((0, 32),), -0.2, 0.2), 0.0, 1.0),
        "obs_value": scatter_about(splits[6], (OBS,), 1.0, 6.0, ((0, 32),), jnp.float32),
        "src_prior": jnp.clip(jnp.exp(math.log(16.0) - 2.7725887 * jax.random.uniform(splits[7], (PARAMS, SOURCES), jnp.float32) ** shard_levels(splits[7], (PARAMS, SOURCES), ((1, 8),), -0.2, 0.2)), 1.0, 16.0),
    }


damping = 0.5
entry_pairs = [(row_at, col_at) for row_at in range(5) for col_at in range(row_at + 1)]

def spline_taps(phase):
    squared = phase * phase
    cubed = squared * phase
    rest = 1.0 - phase
    return (rest * rest * rest / 6.0, (3.0 * cubed - 6.0 * squared + 4.0) / 6.0, (-3.0 * cubed + 3.0 * squared + 3.0 * phase + 1.0) / 6.0, cubed / 6.0)

def factorize(normal):
    factor = {}
    for row_at in range(5):
        for col_at in range(row_at + 1):
            running = normal[row_at, col_at]
            for inner_at in range(col_at):
                running = running - factor[row_at, inner_at] * factor[col_at, inner_at]
            if row_at == col_at:
                factor[row_at, row_at] = jnp.sqrt(running)
            else:
                factor[row_at, col_at] = running / factor[col_at, col_at]
    return factor

def chol_solve(factor, target):
    forward = []
    for row_at in range(5):
        running = target[row_at]
        for inner_at in range(row_at):
            running = running - factor[row_at, inner_at] * forward[inner_at]
        forward.append(running / factor[row_at, row_at])
    result = [None] * 5
    for row_at in reversed(range(5)):
        running = forward[row_at]
        for inner_at in range(row_at + 1, 5):
            running = running - factor[inner_at, row_at] * result[inner_at]
        result[row_at] = running / factor[row_at, row_at]
    return jnp.stack(result)

def source_total(source, rows, count):
    return jnp.zeros((rows.shape[0], count), jnp.float32).at[:, source].add(rows)

def knot_values(padded, knot, design, tap_weights):
    summed = jnp.zeros(knot.shape, jnp.float32)
    for tap_at in range(4):
        picked = jnp.take(padded, knot + tap_at, axis=1)
        summed = summed + tap_weights[tap_at] * lax.optimization_barrier(jnp.sum(design * picked, axis=0))
    return summed

def knot_total(knot, design, tap_weights, weight_vec, extent):
    summed = jnp.zeros((design.shape[0], extent + 3), jnp.float32)
    for tap_at in range(4):
        summed = summed.at[:, knot + tap_at].add(design * (tap_weights[tap_at] * weight_vec))
    return summed

def eliminate(factor, source, design, values_obs, source_sums):
    solved = chol_solve(factor, [source_sums[row_at] for row_at in range(5)])
    fitted = lax.optimization_barrier(jnp.sum(design * jnp.take(solved, source, axis=1), axis=0))
    return values_obs - fitted

def reference(obs_source, obs_knot, obs_count, src_design, att_design, obs_phase, obs_value, src_prior):
    live_mask = (jnp.arange(OBS_DEV, dtype=jnp.int32)[None, :] < obs_count[:, None]).astype(jnp.float32).reshape(-1)
    block_of = jnp.arange(OBS, dtype=jnp.int32) // OBS_DEV
    source = (block_of // N_TM * SRC_DEV + obs_source).astype(jnp.int32)
    knot = (block_of % N_TM * KSEG + obs_knot).astype(jnp.int32)
    src_rows = src_design * live_mask
    att_rows = att_design * live_mask
    observed = obs_value * live_mask
    tap_weights = spline_taps(obs_phase)
    products = jnp.stack([src_rows[row_at] * src_rows[col_at] for row_at, col_at in entry_pairs] + [src_rows[row_at] * observed for row_at in range(5)])
    sums = source_total(source, products, SOURCES)
    normal = {}
    for entry_at, pair in enumerate(entry_pairs):
        normal[pair] = sums[entry_at] + (src_prior[pair[0]] if pair[0] == pair[1] else 0.0)
    factor = factorize(normal)

    def reduced(values_obs, totals):
        cleaned = eliminate(factor, source, src_rows, values_obs, totals)
        return knot_total(knot, att_rows, tap_weights, cleaned, KNOTS)[:, :KNOTS]

    def along_knots(field):
        padded = jnp.concatenate([field, jnp.zeros((4, 3), jnp.float32)], axis=1)
        return knot_values(padded, knot, att_rows, tap_weights)
    residual = reduced(observed, sums[15:])
    solution = jnp.zeros_like(residual)
    direction = residual
    norm_now = jnp.sum(residual * residual)
    for repeat in range(ITERS):
        image_obs = along_knots(direction)
        mapped = reduced(image_obs, source_total(source, src_rows * image_obs, SOURCES)) + damping * direction
        alpha_step = norm_now / jnp.sum(direction * mapped)
        solution = solution + alpha_step * direction
        residual = residual - alpha_step * mapped
        norm_next = jnp.sum(residual * residual)
        direction = residual + norm_next / norm_now * direction
        norm_now = norm_next
    fitted = observed - along_knots(solution)
    source_solution = chol_solve(factor, [row for row in source_total(source, src_rows * fitted, SOURCES)])
    return (solution.reshape(4, N_TM, KSEG), residual.reshape(4, N_TM, KSEG), source_solution)
```

```python
import functools

import jax
import jax.numpy as jnp
from jax import lax
from jax.experimental import pallas as pl
from jax.experimental.pallas import tpu as pltpu
from jax.sharding import PartitionSpec as P

KN_DEV = 256
COMP = 4
TAPS = 4
PAR = 5
LANES = 128
CHUNK = 512

damping = 0.5
entry_pairs = [(row_at, col_at) for row_at in range(PAR) for col_at in range(row_at + 1)]
f32 = jnp.float32
bf16 = jnp.bfloat16


def spline_taps(phase):
    squared = phase * phase
    cubed = squared * phase
    rest = 1.0 - phase
    return (
        rest * rest * rest / 6.0,
        (3.0 * cubed - 6.0 * squared + 4.0) / 6.0,
        (-3.0 * cubed + 3.0 * squared + 3.0 * phase + 1.0) / 6.0,
        cubed / 6.0,
    )


def factorize(normal):
    factor, inverse = {}, {}
    for row_at in range(PAR):
        for col_at in range(row_at + 1):
            running = normal[row_at, col_at]
            for inner_at in range(col_at):
                running = running - factor[row_at, inner_at] * factor[col_at, inner_at]
            if row_at == col_at:
                factor[row_at, row_at] = jnp.sqrt(running)
                inverse[row_at] = 1.0 / factor[row_at, row_at]
            else:
                factor[row_at, col_at] = running * inverse[col_at]
    return factor, inverse


def chol_solve(factor, inverse, target):
    forward = []
    for row_at in range(PAR):
        running = target[row_at]
        for inner_at in range(row_at):
            running = running - factor[row_at, inner_at] * forward[inner_at]
        forward.append(running * inverse[row_at])
    result = [None] * PAR
    for row_at in reversed(range(PAR)):
        running = forward[row_at]
        for inner_at in range(row_at + 1, PAR):
            running = running - factor[inner_at, row_at] * result[inner_at]
        result[row_at] = running * inverse[row_at]
    return result


def two_parts(value):
    high = value.astype(bf16)
    low = (value - high.astype(f32)).astype(bf16)
    return jnp.concatenate([high, low], axis=0)


def joined(value):
    half = value.shape[0] // 2
    return value[:half] + value[half:]


def dot_nn(left, right):
    return lax.dot_general(left, right, (((1,), (0,)), ((), ())), preferred_element_type=f32)


def dot_nt(left, right):
    return lax.dot_general(left, right, (((1,), (1,)), ((), ())), preferred_element_type=f32)


def kernel(
    n_sky, n_tm,
    source_ref, knot_ref, count_ref, src_ref, att_ref, phase_ref, value_ref, prior_ref,
    sol_ref, res_ref, out_ref,
    hot_k, hot_s, rows_k, rows_s, y_ref, u0_ref, u1_ref,
    acc_a, acc_s, acc_k, taps_ref, z_ref,
    buf_a, buf_t, buf_c, buf_f, buf_p, buf_n,
    field_b, field_r, field_p, field_x,
    ss_t, rs_t, ss_f, rs_f, ss_p, rs_p, ss_n, rs_n,
):
    me_s = lax.axis_index("sky")
    me_t = lax.axis_index("tm")
    slots = source_ref.shape[1]
    hk = n_sky
    hs = prior_ref.shape[1] // LANES
    main = COMP * hk
    chunks = slots // CHUNK

    barrier = pltpu.get_barrier_semaphore()
    for ds in range(n_sky):
        for dt in range(n_tm):
            if ds or dt:
                pl.semaphore_signal(
                    barrier, inc=1,
                    device_id={"sky": lax.rem(me_s + ds, n_sky), "tm": lax.rem(me_t + dt, n_tm)},
                    device_id_type=pl.DeviceIdType.MESH,
                )

    def span(at):
        return pl.ds(pl.multiple_of(at * CHUNK, CHUNK), CHUNK)

    acc_a[...] = jnp.zeros_like(acc_a)

    def prepare(at, _):
        here = span(at)
        lane = lax.broadcasted_iota(jnp.int32, (1, CHUNK), 1) + at * CHUNK
        live = (lane < count_ref[0]).astype(f32)
        knot, source = knot_ref[:, here], source_ref[:, here]
        knot_low, knot_high = knot & (KN_DEV - 1), knot >> 8
        src_low, src_high = source & (LANES - 1), source >> 7
        hot_k[:, here] = (
            lax.broadcasted_iota(jnp.int32, (KN_DEV, CHUNK), 0) == knot_low
        ).astype(f32).astype(bf16)
        hot_s_here = (
            lax.broadcasted_iota(jnp.int32, (LANES, CHUNK), 0) == src_low
        ).astype(f32).astype(bf16)
        hot_s[:, here] = hot_s_here
        mask_k = (lax.broadcasted_iota(jnp.int32, (hk, CHUNK), 0) == knot_high).astype(f32)
        mask_s = (lax.broadcasted_iota(jnp.int32, (hs, CHUNK), 0) == src_high).astype(f32)
        weights = spline_taps(phase_ref[:, here])
        observed = value_ref[:, here] * live
        y_ref[:, here] = observed
        for c in range(COMP):
            design = att_ref[c : c + 1, here] * live
            for m in range(TAPS):
                base = (c * TAPS + m) * hk
                rows_k[base : base + hk, here] = mask_k * (design * weights[m])
        designs = [src_ref[e : e + 1, here] * live for e in range(PAR)]
        masked = [mask_s * design for design in designs]
        for e in range(PAR):
            rows_s[e * hs : (e + 1) * hs, here] = masked[e]
        products = jnp.concatenate(
            [masked[i] * designs[j] for i, j in entry_pairs]
            + [masked[e] * observed for e in range(PAR)],
            axis=0,
        )
        acc_a[...] += dot_nt(two_parts(products), hot_s_here)
        return 0

    lax.fori_loop(0, chunks, prepare, 0)

    def over_tm(buf, stage):
        copies = []
        for d in range(1, n_tm):
            copy = pltpu.make_async_remote_copy(
                src_ref=buf.at[me_t], dst_ref=buf.at[me_t],
                send_sem=ss_t.at[stage, d - 1], recv_sem=rs_t.at[stage, d - 1],
                device_id={"sky": me_s, "tm": lax.rem(me_t + d, n_tm)},
                device_id_type=pl.DeviceIdType.MESH,
            )
            copy.start()
            copies.append(copy)
        for copy in copies:
            copy.wait()

    def over_sky(stage):
        mine = buf_f.at[stage, me_s]
        edge = buf_f.at[stage, me_s, pl.ds(main, 8)]
        copies = []
        for ds in range(1, n_sky):
            copies.append(pltpu.make_async_remote_copy(
                src_ref=mine, dst_ref=mine,
                send_sem=ss_f.at[stage, ds - 1], recv_sem=rs_f.at[stage, ds - 1],
                device_id={"sky": lax.rem(me_s + ds, n_sky), "tm": me_t},
                device_id_type=pl.DeviceIdType.MESH,
            ))
        for ds in range(n_sky):
            copies.append(pltpu.make_async_remote_copy(
                src_ref=edge, dst_ref=buf_p.at[stage, me_s],
                send_sem=ss_p.at[stage, ds], recv_sem=rs_p.at[stage, ds],
                device_id={"sky": lax.rem(me_s + ds, n_sky), "tm": lax.rem(me_t + 1, n_tm)},
                device_id_type=pl.DeviceIdType.MESH,
            ))
            copies.append(pltpu.make_async_remote_copy(
                src_ref=edge, dst_ref=buf_n.at[stage, me_s],
                send_sem=ss_n.at[stage, ds], recv_sem=rs_n.at[stage, ds],
                device_id={"sky": lax.rem(me_s + ds, n_sky), "tm": lax.rem(me_t + n_tm - 1, n_tm)},
                device_id_type=pl.DeviceIdType.MESH,
            ))
        for copy in copies:
            copy.start()
        for copy in copies:
            copy.wait()

    def added(buf, count):
        total = buf[0]
        for at in range(1, count):
            total = total + buf[at]
        return total

    def elimination(v_of, stage):
        acc_k[...] = jnp.zeros_like(acc_k)

        def step(at, _):
            here = span(at)
            picked = joined(dot_nn(z_ref[...], hot_s[:, here]))
            fitted = jnp.sum(rows_s[:, here] * picked, axis=0, keepdims=True)
            cleaned = v_of(here) - fitted
            acc_k[...] += dot_nt(two_parts(rows_k[:, here] * cleaned), hot_k[:, here])
            return 0

        lax.fori_loop(0, chunks, step, 0)
        lane = lax.broadcasted_iota(jnp.int32, (hk, KN_DEV), 1)
        row = lax.broadcasted_iota(jnp.int32, (hk, KN_DEV), 0)
        pairs = TAPS * COMP * hk
        blocks, overs, firsts = [], [], []
        for c in range(COMP):
            block, over = None, None
            for m in range(TAPS):
                base = (c * TAPS + m) * hk
                part = acc_k[base : base + hk, :] + acc_k[pairs + base : pairs + base + hk, :]
                if m == 0:
                    block = part
                    continue
                turned = pltpu.roll(part, m, 1)
                above = pltpu.roll(turned, 1, 0)
                block = block + jnp.where(lane >= m, turned, jnp.where(row > 0, above, 0.0))
                past = jnp.where(lane[:1] < m, above[:1], 0.0)
                over = past if over is None else over + past
            blocks.append(block)
            overs.append(over)
            firsts.append(block[:1])
        buf_f[stage, me_s] = jnp.concatenate(blocks + overs + firsts, axis=0)

    def knot_field(stage):
        total = added(buf_f.at[stage], n_sky)
        before = added(buf_p.at[stage], n_sky)
        after = added(buf_n.at[stage], n_sky)
        lane = lax.broadcasted_iota(jnp.int32, (hk, KN_DEV), 1)
        row = lax.broadcasted_iota(jnp.int32, (hk, KN_DEV), 0)
        has_before = (me_t > 0).astype(f32)
        has_after = (me_t < n_tm - 1).astype(f32)
        corner = jnp.logical_and(lane < TAPS - 1, row == 0)
        blocks = []
        for c in range(COMP):
            block = total[c * hk : (c + 1) * hk]
            blocks.append(block + jnp.where(corner, before[c : c + 1] * has_before, 0.0))
        edge = (total[main : main + COMP] + after[COMP : 2 * COMP]) * has_after
        edge = jnp.where(lax.broadcasted_iota(jnp.int32, edge.shape, 1) < TAPS - 1, edge, 0.0)
        return jnp.concatenate(blocks + [edge, jnp.zeros_like(edge)], axis=0)

    def along_knots(field, u_ref):
        lane = lax.broadcasted_iota(jnp.int32, (hk, KN_DEV), 1)
        row = lax.broadcasted_iota(jnp.int32, (hk, KN_DEV), 0)
        shifts = []
        for c in range(COMP):
            block = field[c * hk : (c + 1) * hk]
            below = jnp.where(row == hk - 1, field[main + c : main + c + 1], pltpu.roll(block, hk - 1, 0))
            shifts.append(block)
            for m in range(1, TAPS):
                shifts.append(pltpu.roll(jnp.where(lane < m, below, block), KN_DEV - m, 1))
        taps_ref[...] = two_parts(jnp.concatenate(shifts, axis=0))
        acc_s[...] = jnp.zeros_like(acc_s)

        def step(at, _):
            here = span(at)
            picked = joined(dot_nn(taps_ref[...], hot_k[:, here]))
            mapped = jnp.sum(rows_k[:, here] * picked, axis=0, keepdims=True)
            u_ref[:, here] = mapped
            acc_s[...] += dot_nt(two_parts(rows_s[:, here] * mapped), hot_s[:, here])
            return 0

        lax.fori_loop(0, chunks, step, 0)
        return joined(acc_s[...])

    def tiles(value):
        return [value[e * hs : (e + 1) * hs] for e in range(PAR)]

    def scalars(*values):
        row = lax.broadcasted_iota(jnp.int32, (8, LANES), 0)
        tile = jnp.zeros((8, LANES), f32)
        for at, value in enumerate(values):
            tile = jnp.where(row == at, value, tile)
        return tile

    def inner(left, right):
        return jnp.sum(left[:main] * right[:main])

    buf_a[me_t] = joined(acc_a[...])
    pl.semaphore_wait(barrier, n_sky * n_tm - 1)
    over_tm(buf_a, 0)
    sums = added(buf_a, n_tm)
    normal = {}
    for entry_at, pair in enumerate(entry_pairs):
        entry = sums[entry_at * hs : (entry_at + 1) * hs]
        if pair[0] == pair[1]:
            e = pair[0]
            entry = entry + jnp.concatenate(
                [prior_ref[e : e + 1, h * LANES : (h + 1) * LANES] for h in range(hs)], axis=0
            )
        normal[pair] = entry
    factor, inverse = factorize(normal)
    sums_y = sums[len(entry_pairs) * hs :]

    def solved(value):
        return chol_solve(factor, inverse, tiles(value))

    def solve_into_z(value):
        z_ref[...] = two_parts(jnp.concatenate(solved(value), axis=0))

    solve_into_z(sums_y)
    elimination(lambda here: y_ref[:, here], 0)
    over_sky(0)
    field_b[...] = knot_field(0)

    size = PAR * hs
    buf_t[0, me_t, :size, :] = along_knots(field_b[...], u0_ref)
    over_tm(buf_t.at[0], 1)
    sums_0 = added(buf_t.at[0], n_tm)[:size]
    solve_into_z(sums_0)
    elimination(lambda here: u0_ref[:, here], 1)
    over_sky(1)
    b = field_b[...]
    q = knot_field(1) + damping * b
    field_x[...] = q

    buf_t[1, me_t, :size, :] = along_knots(q, u1_ref)
    buf_t[1, me_t, size:, :] = scalars(inner(b, b), inner(b, q), inner(q, q))
    over_tm(buf_t.at[1], 2)
    total = added(buf_t.at[1], n_tm)
    norm_0, b_q, q_q = (total[size + at : size + at + 1, :1] for at in range(3))
    alpha_0 = norm_0 / b_q
    norm_1 = norm_0 - alpha_0 * (2.0 * b_q - alpha_0 * q_q)
    beta_0 = norm_1 / norm_0
    sums_1 = (1.0 + beta_0) * sums_0 - alpha_0 * total[:size]
    solve_into_z(sums_1)
    residual = field_b[...] - alpha_0 * field_x[...]
    field_r[...] = residual
    field_p[...] = residual + beta_0 * field_b[...]
    elimination(lambda here: (1.0 + beta_0) * u0_ref[:, here] - alpha_0 * u1_ref[:, here], 2)
    over_sky(2)
    direction = field_p[...]
    q = knot_field(2) + damping * direction
    residual = field_r[...]
    buf_c[me_t] = scalars(inner(residual, residual), inner(direction, q))
    over_tm(buf_c, 3)
    total = added(buf_c, n_tm)
    alpha_1 = total[0:1, :1] / total[1:2, :1]
    field_x[...] = alpha_0 * field_b[...] + alpha_1 * direction
    field_r[...] = residual - alpha_1 * q
    for c in range(COMP):
        sol_ref[c] = field_x[pl.ds(c * hk + me_s, 1), :]
        res_ref[c] = field_r[pl.ds(c * hk + me_s, 1), :]
    last = solved(sums_y - alpha_0 * sums_0 - alpha_1 * sums_1)
    for e in range(PAR):
        for h in range(hs):
            out_ref[e : e + 1, h * LANES : (h + 1) * LANES] = last[e][h : h + 1]


def solution(mesh):
    n_sky, n_tm = mesh.shape["sky"], mesh.shape["tm"]

    def shards(obs_source, obs_knot, obs_count, src_design, att_design, obs_phase, obs_value, src_prior):
        slots = obs_source.shape[0]
        hk, hs = n_sky, src_prior.shape[1] // LANES
        pairs = COMP * TAPS * hk
        main = COMP * hk
        entries = len(entry_pairs) + PAR
        vmem = pl.BlockSpec(memory_space=pltpu.VMEM)
        smem = pl.BlockSpec(memory_space=pltpu.SMEM)
        dma = pltpu.SemaphoreType.DMA
        return pl.pallas_call(
            functools.partial(kernel, n_sky, n_tm),
            out_shape=(
                jax.ShapeDtypeStruct((COMP, 1, KN_DEV), f32),
                jax.ShapeDtypeStruct((COMP, 1, KN_DEV), f32),
                jax.ShapeDtypeStruct(src_prior.shape, f32),
            ),
            in_specs=[vmem, vmem, smem, vmem, vmem, vmem, vmem, vmem],
            out_specs=(vmem, vmem, vmem),
            scratch_shapes=[
                pltpu.VMEM((KN_DEV, slots), bf16),
                pltpu.VMEM((LANES, slots), bf16),
                pltpu.VMEM((pairs, slots), f32),
                pltpu.VMEM((PAR * hs, slots), f32),
                pltpu.VMEM((1, slots), f32),
                pltpu.VMEM((1, slots), f32),
                pltpu.VMEM((1, slots), f32),
                pltpu.VMEM((2 * entries * hs, LANES), f32),
                pltpu.VMEM((2 * PAR * hs, LANES), f32),
                pltpu.VMEM((2 * pairs, KN_DEV), f32),
                pltpu.VMEM((2 * pairs, KN_DEV), bf16),
                pltpu.VMEM((2 * PAR * hs, LANES), bf16),
                pltpu.VMEM((n_tm, entries * hs, LANES), f32),
                pltpu.VMEM((2, n_tm, PAR * hs + 8, LANES), f32),
                pltpu.VMEM((n_tm, 8, LANES), f32),
                pltpu.VMEM((3, n_sky, main + 8, KN_DEV), f32),
                pltpu.VMEM((3, n_sky, 8, KN_DEV), f32),
                pltpu.VMEM((3, n_sky, 8, KN_DEV), f32),
                pltpu.VMEM((main + 8, KN_DEV), f32),
                pltpu.VMEM((main + 8, KN_DEV), f32),
                pltpu.VMEM((main + 8, KN_DEV), f32),
                pltpu.VMEM((main + 8, KN_DEV), f32),
                dma((4, n_tm - 1)), dma((4, n_tm - 1)),
                dma((3, n_sky - 1)), dma((3, n_sky - 1)),
                dma((3, n_sky)), dma((3, n_sky)),
                dma((3, n_sky)), dma((3, n_sky)),
            ],
            compiler_params=pltpu.CompilerParams(collective_id=0, has_side_effects=True),
        )(
            obs_source.reshape(1, slots), obs_knot.reshape(1, slots), obs_count,
            src_design, att_design, obs_phase.reshape(1, slots), obs_value.reshape(1, slots), src_prior,
        )

    placed = (
        P(("sky", "tm")),
        P(("sky", "tm")),
        P(("sky", "tm")),
        P(None, ("sky", "tm")),
        P(None, ("sky", "tm")),
        P(("sky", "tm")),
        P(("sky", "tm")),
        P(None, "sky"),
    )
    return jax.shard_map(
        shards,
        mesh=mesh,
        in_specs=placed,
        out_specs=(P(None, "tm", "sky"), P(None, "tm", "sky"), P(None, "sky")),
        check_vma=False,
    )
```

```python
import functools

import jax
import jax.numpy as jnp
from jax import lax
from jax.experimental import pallas as pl
from jax.experimental.pallas import tpu as pltpu
from jax.sharding import PartitionSpec as P

KN_DEV = 256
COMP = 4
TAPS = 4
PAR = 5
LANES = 128
CHUNK = 2048
SCALAR = 64

damping = 0.5
entry_pairs = [(row_at, col_at) for row_at in range(PAR) for col_at in range(row_at + 1)]
f32 = jnp.float32
bf16 = jnp.bfloat16


def spline_taps(phase):
    squared = phase * phase
    cubed = squared * phase
    rest = 1.0 - phase
    return (
        rest * rest * rest / 6.0,
        (3.0 * cubed - 6.0 * squared + 4.0) / 6.0,
        (-3.0 * cubed + 3.0 * squared + 3.0 * phase + 1.0) / 6.0,
        cubed / 6.0,
    )


def factorize(normal):
    factor, inverse = {}, {}
    for row_at in range(PAR):
        for col_at in range(row_at + 1):
            running = normal[row_at, col_at]
            for inner_at in range(col_at):
                running = running - factor[row_at, inner_at] * factor[col_at, inner_at]
            if row_at == col_at:
                factor[row_at, row_at] = jnp.sqrt(running)
                inverse[row_at] = 1.0 / factor[row_at, row_at]
            else:
                factor[row_at, col_at] = running * inverse[col_at]
    return factor, inverse


def chol_solve(factor, inverse, target):
    forward = []
    for row_at in range(PAR):
        running = target[row_at]
        for inner_at in range(row_at):
            running = running - factor[row_at, inner_at] * forward[inner_at]
        forward.append(running * inverse[row_at])
    result = [None] * PAR
    for row_at in reversed(range(PAR)):
        running = forward[row_at]
        for inner_at in range(row_at + 1, PAR):
            running = running - factor[inner_at, row_at] * result[inner_at]
        result[row_at] = running * inverse[row_at]
    return result


def two_parts(value):
    high = value.astype(bf16)
    low = (value - high.astype(f32)).astype(bf16)
    return jnp.concatenate([high, low], axis=0)


def joined(value):
    half = value.shape[0] // 2
    return value[:half] + value[half:]


def dot_nn(left, right):
    return lax.dot_general(left, right, (((1,), (0,)), ((), ())), preferred_element_type=f32)


def dot_nt(left, right):
    return lax.dot_general(left, right, (((1,), (1,)), ((), ())), preferred_element_type=f32)


def kernel(
    n_sky, n_tm,
    source_ref, knot_ref, count_ref, src_ref, att_ref, phase_ref, value_ref, prior_ref,
    sol_ref, res_ref, out_ref,
    hot_k, hot_s, rows_k, rows_s, y_ref, u0_ref, u1_ref,
    acc_a, acc_s, acc_k, taps_ref, z_ref,
    buf_a, buf_t, buf_f, buf_e,
    field_b, field_r, field_p, field_x,
    ss_t, rs_t, ss_f, rs_f, ss_e, rs_e,
):
    me_s = lax.axis_index("sky")
    me_t = lax.axis_index("tm")
    slots = source_ref.shape[1]
    hk = n_sky
    hs = prior_ref.shape[1] // LANES
    main = COMP * hk
    chunks = slots // CHUNK

    barrier = pltpu.get_barrier_semaphore()
    for ds in range(n_sky):
        for dt in range(n_tm):
            if ds or dt:
                pl.semaphore_signal(
                    barrier, inc=1,
                    device_id={"sky": lax.rem(me_s + ds, n_sky), "tm": lax.rem(me_t + dt, n_tm)},
                    device_id_type=pl.DeviceIdType.MESH,
                )

    def span(at):
        return pl.ds(pl.multiple_of(at * CHUNK, CHUNK), CHUNK)

    acc_a[...] = jnp.zeros_like(acc_a)

    def prepare(at, _):
        here = span(at)
        lane = lax.broadcasted_iota(jnp.int32, (1, CHUNK), 1) + at * CHUNK
        live = (lane < count_ref[0]).astype(f32)
        source = source_ref[:, here]
        src_low, src_high = source & (LANES - 1), source >> 7
        hot_s_here = (
            lax.broadcasted_iota(jnp.int32, (LANES, CHUNK), 0) == src_low
        ).astype(f32).astype(bf16)
        hot_s[:, here] = hot_s_here
        mask_s = (lax.broadcasted_iota(jnp.int32, (hs, CHUNK), 0) == src_high).astype(f32)
        observed = value_ref[:, here] * live
        y_ref[:, here] = observed
        designs = [src_ref[e : e + 1, here] * live for e in range(PAR)]
        masked = [mask_s * design for design in designs]
        for e in range(PAR):
            rows_s[e * hs : (e + 1) * hs, here] = masked[e]
        products = jnp.concatenate(
            [masked[i] * designs[j] for i, j in entry_pairs]
            + [masked[e] * observed for e in range(PAR)],
            axis=0,
        )
        acc_a[...] += dot_nt(two_parts(products), hot_s_here)
        return 0

    lax.fori_loop(0, chunks, prepare, 0)

    def prepare_knots(at, _):
        here = span(at)
        lane = lax.broadcasted_iota(jnp.int32, (1, CHUNK), 1) + at * CHUNK
        live = (lane < count_ref[0]).astype(f32)
        knot = knot_ref[:, here]
        knot_low, knot_high = knot & (KN_DEV - 1), knot >> 8
        hot_k[:, here] = (
            lax.broadcasted_iota(jnp.int32, (KN_DEV, CHUNK), 0) == knot_low
        ).astype(f32).astype(bf16)
        mask_k = (lax.broadcasted_iota(jnp.int32, (hk, CHUNK), 0) == knot_high).astype(f32)
        weights = spline_taps(phase_ref[:, here])
        for c in range(COMP):
            design = att_ref[c : c + 1, here] * live
            for m in range(TAPS):
                base = (c * TAPS + m) * hk
                rows_k[base : base + hk, here] = mask_k * (design * weights[m])
        return 0

    def over_tm(buf, stage):
        copies = []
        for d in range(1, n_tm):
            copy = pltpu.make_async_remote_copy(
                src_ref=buf.at[me_t], dst_ref=buf.at[me_t],
                send_sem=ss_t.at[stage, d - 1], recv_sem=rs_t.at[stage, d - 1],
                device_id={"sky": me_s, "tm": lax.rem(me_t + d, n_tm)},
                device_id_type=pl.DeviceIdType.MESH,
            )
            copy.start()
            copies.append(copy)
        return copies

    def finish(copies):
        for copy in copies:
            copy.wait()

    def edge_offsets(stage):
        return range(n_tm) if stage == 2 else sorted({0, 1, n_tm - 1})

    def over_sky(stage):
        mine = buf_f.at[stage, me_s]
        row = buf_e.at[stage, me_t, me_s]
        copies = []
        for ds in range(1, n_sky):
            copies.append(pltpu.make_async_remote_copy(
                src_ref=mine, dst_ref=mine,
                send_sem=ss_f.at[stage, ds - 1], recv_sem=rs_f.at[stage, ds - 1],
                device_id={"sky": lax.rem(me_s + ds, n_sky), "tm": me_t},
                device_id_type=pl.DeviceIdType.MESH,
            ))
        for dt in edge_offsets(stage):
            for ds in range(n_sky):
                if ds or dt:
                    copies.append(pltpu.make_async_remote_copy(
                        src_ref=row, dst_ref=row,
                        send_sem=ss_e.at[stage, dt, ds], recv_sem=rs_e.at[stage, dt, ds],
                        device_id={"sky": lax.rem(me_s + ds, n_sky), "tm": lax.rem(me_t + dt, n_tm)},
                        device_id_type=pl.DeviceIdType.MESH,
                    ))
        for copy in copies:
            copy.start()
        for copy in copies:
            copy.wait()

    def added(buf, count):
        total = buf[0]
        for at in range(1, count):
            total = total + buf[at]
        return total

    def elimination(v_of, stage):
        acc_k[...] = jnp.zeros_like(acc_k)

        def step(at, energy):
            here = span(at)
            picked = joined(dot_nn(z_ref[...], hot_s[:, here]))
            fitted = jnp.sum(rows_s[:, here] * picked, axis=0, keepdims=True)
            value = v_of(here)
            cleaned = value - fitted
            acc_k[...] += dot_nt(two_parts(rows_k[:, here] * cleaned), hot_k[:, here])
            return energy + value * cleaned

        energy = lax.fori_loop(0, chunks, step, jnp.zeros((1, CHUNK), f32))
        lane = lax.broadcasted_iota(jnp.int32, (hk, KN_DEV), 1)
        row = lax.broadcasted_iota(jnp.int32, (hk, KN_DEV), 0)
        pairs = TAPS * COMP * hk
        blocks, overs, firsts = [], [], []
        for c in range(COMP):
            block, over = None, None
            for m in range(TAPS):
                base = (c * TAPS + m) * hk
                part = acc_k[base : base + hk, :] + acc_k[pairs + base : pairs + base + hk, :]
                if m == 0:
                    block = part
                    continue
                turned = pltpu.roll(part, m, 1)
                above = pltpu.roll(turned, 1, 0)
                block = block + jnp.where(lane >= m, turned, jnp.where(row > 0, above, 0.0))
                past = jnp.where(lane[:1] < m, above[:1], 0.0)
                over = past if over is None else over + past
            blocks.append(block)
            overs.append(over)
            firsts.append(block[:1])
        buf_f[stage, me_s] = jnp.concatenate(blocks, axis=0)
        edge_lane = lax.broadcasted_iota(jnp.int32, (1, LANES), 1)
        packed = jnp.where(edge_lane == SCALAR, jnp.sum(energy, axis=1, keepdims=True), 0.0)
        for c in range(COMP):
            past = jnp.where(edge_lane < TAPS - 1, overs[c][:, :LANES], 0.0)
            first = jnp.where(edge_lane < TAPS - 1, firsts[c][:, :LANES], 0.0)
            packed = packed + (pltpu.roll(past, 8 * c, 1) if c else past) + pltpu.roll(first, 8 * (COMP + c), 1)
        buf_e[stage, me_t, me_s] = packed

    def knot_field(stage):
        total = added(buf_f.at[stage], n_sky)
        own = added(buf_e.at[stage, me_t], n_sky)
        before = added(buf_e.at[stage, lax.rem(me_t + n_tm - 1, n_tm)], n_sky)
        after = added(buf_e.at[stage, lax.rem(me_t + 1, n_tm)], n_sky)
        edge_lane = lax.broadcasted_iota(jnp.int32, (1, LANES), 1)
        rest = jnp.zeros((1, KN_DEV - LANES), f32)

        def unpacked(packed, at):
            turned = pltpu.roll(packed, LANES - 8 * at, 1) if at else packed
            return jnp.concatenate([jnp.where(edge_lane < TAPS - 1, turned, 0.0), rest], axis=1)

        lane = lax.broadcasted_iota(jnp.int32, (hk, KN_DEV), 1)
        row = lax.broadcasted_iota(jnp.int32, (hk, KN_DEV), 0)
        has_before = (me_t > 0).astype(f32)
        has_after = (me_t < n_tm - 1).astype(f32)
        corner = jnp.logical_and(lane < TAPS - 1, row == 0)
        blocks = []
        for c in range(COMP):
            block = total[c * hk : (c + 1) * hk]
            blocks.append(block + jnp.where(corner, unpacked(before, c) * has_before, 0.0))
        edge = jnp.concatenate(
            [(unpacked(own, c) + unpacked(after, COMP + c)) * has_after for c in range(COMP)], axis=0
        )
        return jnp.concatenate(blocks + [edge, jnp.zeros_like(edge)], axis=0)

    def along_knots(field, u_ref):
        lane = lax.broadcasted_iota(jnp.int32, (hk, KN_DEV), 1)
        row = lax.broadcasted_iota(jnp.int32, (hk, KN_DEV), 0)
        shifts = []
        for c in range(COMP):
            block = field[c * hk : (c + 1) * hk]
            below = jnp.where(row == hk - 1, field[main + c : main + c + 1], pltpu.roll(block, hk - 1, 0))
            shifts.append(block)
            for m in range(1, TAPS):
                shifts.append(pltpu.roll(jnp.where(lane < m, below, block), KN_DEV - m, 1))
        taps_ref[...] = two_parts(jnp.concatenate(shifts, axis=0))
        acc_s[...] = jnp.zeros_like(acc_s)

        def step(at, _):
            here = span(at)
            picked = joined(dot_nn(taps_ref[...], hot_k[:, here]))
            mapped = jnp.sum(rows_k[:, here] * picked, axis=0, keepdims=True)
            u_ref[:, here] = mapped
            acc_s[...] += dot_nt(two_parts(rows_s[:, here] * mapped), hot_s[:, here])
            return 0

        lax.fori_loop(0, chunks, step, 0)
        return joined(acc_s[...])

    def tiles(value):
        return [value[e * hs : (e + 1) * hs] for e in range(PAR)]

    def scalars(*values):
        row = lax.broadcasted_iota(jnp.int32, (8, LANES), 0)
        tile = jnp.zeros((8, LANES), f32)
        for at, value in enumerate(values):
            tile = jnp.where(row == at, value, tile)
        return tile

    def inner(left, right):
        return jnp.sum(left[:main] * right[:main])

    buf_a[me_t] = joined(acc_a[...])
    pl.semaphore_wait(barrier, n_sky * n_tm - 1)
    copies = over_tm(buf_a, 0)
    lax.fori_loop(0, chunks, prepare_knots, 0)
    finish(copies)
    sums = added(buf_a, n_tm)
    normal = {}
    for entry_at, pair in enumerate(entry_pairs):
        entry = sums[entry_at * hs : (entry_at + 1) * hs]
        if pair[0] == pair[1]:
            e = pair[0]
            entry = entry + jnp.concatenate(
                [prior_ref[e : e + 1, h * LANES : (h + 1) * LANES] for h in range(hs)], axis=0
            )
        normal[pair] = entry
    factor, inverse = factorize(normal)
    sums_y = sums[len(entry_pairs) * hs :]

    def solved(value):
        return chol_solve(factor, inverse, tiles(value))

    def solve_into_z(value):
        z_ref[...] = two_parts(jnp.concatenate(solved(value), axis=0))

    solve_into_z(sums_y)
    elimination(lambda here: y_ref[:, here], 0)
    over_sky(0)
    field_b[...] = knot_field(0)

    size = PAR * hs
    buf_t[0, me_t, :size, :] = along_knots(field_b[...], u0_ref)
    finish(over_tm(buf_t.at[0, :, pl.ds(0, size)], 1))
    sums_0 = added(buf_t.at[0, :, pl.ds(0, size)], n_tm)
    solve_into_z(sums_0)
    elimination(lambda here: u0_ref[:, here], 1)
    over_sky(1)
    b = field_b[...]
    q = knot_field(1) + damping * b
    field_x[...] = q

    buf_t[1, me_t, :size, :] = along_knots(q, u1_ref)
    buf_t[1, me_t, size:, :] = scalars(inner(b, b), inner(b, q), inner(q, q))
    finish(over_tm(buf_t.at[1], 2))
    total = added(buf_t.at[1], n_tm)
    norm_0, b_q, q_q = (total[size + at : size + at + 1, :1] for at in range(3))
    alpha_0 = norm_0 / b_q
    norm_1 = norm_0 - alpha_0 * (2.0 * b_q - alpha_0 * q_q)
    beta_0 = norm_1 / norm_0
    sums_1 = (1.0 + beta_0) * sums_0 - alpha_0 * total[:size]
    solve_into_z(sums_1)
    residual = field_b[...] - alpha_0 * field_x[...]
    field_r[...] = residual
    field_p[...] = residual + beta_0 * field_b[...]
    elimination(lambda here: (1.0 + beta_0) * u0_ref[:, here] - alpha_0 * u1_ref[:, here], 2)
    over_sky(2)
    direction = field_p[...]
    q = knot_field(2) + damping * direction
    residual = field_r[...]
    energy = added(buf_e.at[2, 0], n_sky)
    for t in range(1, n_tm):
        energy = energy + added(buf_e.at[2, t], n_sky)
    alpha_1 = norm_1 / (energy[:, SCALAR : SCALAR + 1] + damping * (1.0 + beta_0) * norm_1)
    field_x[...] = alpha_0 * field_b[...] + alpha_1 * direction
    field_r[...] = residual - alpha_1 * q
    for c in range(COMP):
        sol_ref[c] = field_x[pl.ds(c * hk + me_s, 1), :]
        res_ref[c] = field_r[pl.ds(c * hk + me_s, 1), :]
    last = solved(sums_y - alpha_0 * sums_0 - alpha_1 * sums_1)
    for e in range(PAR):
        for h in range(hs):
            out_ref[e : e + 1, h * LANES : (h + 1) * LANES] = last[e][h : h + 1]


def solution(mesh):
    n_sky, n_tm = mesh.shape["sky"], mesh.shape["tm"]

    def shards(obs_source, obs_knot, obs_count, src_design, att_design, obs_phase, obs_value, src_prior):
        slots = obs_source.shape[0]
        hk, hs = n_sky, src_prior.shape[1] // LANES
        pairs = COMP * TAPS * hk
        main = COMP * hk
        entries = len(entry_pairs) + PAR
        vmem = pl.BlockSpec(memory_space=pltpu.VMEM)
        smem = pl.BlockSpec(memory_space=pltpu.SMEM)
        dma = pltpu.SemaphoreType.DMA
        return pl.pallas_call(
            functools.partial(kernel, n_sky, n_tm),
            out_shape=(
                jax.ShapeDtypeStruct((COMP, 1, KN_DEV), f32),
                jax.ShapeDtypeStruct((COMP, 1, KN_DEV), f32),
                jax.ShapeDtypeStruct(src_prior.shape, f32),
            ),
            in_specs=[vmem, vmem, smem, vmem, vmem, vmem, vmem, vmem],
            out_specs=(vmem, vmem, vmem),
            scratch_shapes=[
                pltpu.VMEM((KN_DEV, slots), bf16),
                pltpu.VMEM((LANES, slots), bf16),
                pltpu.VMEM((pairs, slots), f32),
                pltpu.VMEM((PAR * hs, slots), f32),
                pltpu.VMEM((1, slots), f32),
                pltpu.VMEM((1, slots), f32),
                pltpu.VMEM((1, slots), f32),
                pltpu.VMEM((2 * entries * hs, LANES), f32),
                pltpu.VMEM((2 * PAR * hs, LANES), f32),
                pltpu.VMEM((2 * pairs, KN_DEV), f32),
                pltpu.VMEM((2 * pairs, KN_DEV), bf16),
                pltpu.VMEM((2 * PAR * hs, LANES), bf16),
                pltpu.VMEM((n_tm, entries * hs, LANES), f32),
                pltpu.VMEM((2, n_tm, PAR * hs + 8, LANES), f32),
                pltpu.VMEM((3, n_sky, main, KN_DEV), f32),
                pltpu.VMEM((3, n_tm, n_sky, 1, LANES), f32),
                pltpu.VMEM((main + 8, KN_DEV), f32),
                pltpu.VMEM((main + 8, KN_DEV), f32),
                pltpu.VMEM((main + 8, KN_DEV), f32),
                pltpu.VMEM((main + 8, KN_DEV), f32),
                dma((3, n_tm - 1)), dma((3, n_tm - 1)),
                dma((3, n_sky - 1)), dma((3, n_sky - 1)),
                dma((3, n_tm, n_sky)), dma((3, n_tm, n_sky)),
            ],
            compiler_params=pltpu.CompilerParams(collective_id=0, has_side_effects=True),
        )(
            obs_source.reshape(1, slots), obs_knot.reshape(1, slots), obs_count,
            src_design, att_design, obs_phase.reshape(1, slots), obs_value.reshape(1, slots), src_prior,
        )

    placed = (
        P(("sky", "tm")),
        P(("sky", "tm")),
        P(("sky", "tm")),
        P(None, ("sky", "tm")),
        P(None, ("sky", "tm")),
        P(("sky", "tm")),
        P(("sky", "tm")),
        P(None, "sky"),
    )
    return jax.shard_map(
        shards,
        mesh=mesh,
        in_specs=placed,
        out_specs=(P(None, "tm", "sky"), P(None, "tm", "sky"), P(None, "sky")),
        check_vma=False,
    )
```

```python
import functools

import jax
import jax.numpy as jnp
from jax import lax
from jax.experimental import pallas as pl
from jax.experimental.pallas import tpu as pltpu
from jax.sharding import PartitionSpec as P

KN_DEV = 256
COMP = 4
TAPS = 4
PAR = 5
LANES = 128
CHUNK = 2048
SCALAR = 64

damping = 0.5
entry_pairs = [(row_at, col_at) for row_at in range(PAR) for col_at in range(row_at + 1)]
f32 = jnp.float32
bf16 = jnp.bfloat16


def spline_taps(phase):
    squared = phase * phase
    cubed = squared * phase
    rest = 1.0 - phase
    return (
        rest * rest * rest / 6.0,
        (3.0 * cubed - 6.0 * squared + 4.0) / 6.0,
        (-3.0 * cubed + 3.0 * squared + 3.0 * phase + 1.0) / 6.0,
        cubed / 6.0,
    )


def factorize(normal):
    factor, inverse = {}, {}
    for row_at in range(PAR):
        for col_at in range(row_at + 1):
            running = normal[row_at, col_at]
            for inner_at in range(col_at):
                running = running - factor[row_at, inner_at] * factor[col_at, inner_at]
            if row_at == col_at:
                factor[row_at, row_at] = jnp.sqrt(running)
                inverse[row_at] = 1.0 / factor[row_at, row_at]
            else:
                factor[row_at, col_at] = running * inverse[col_at]
    return factor, inverse


def chol_solve(factor, inverse, target):
    forward = []
    for row_at in range(PAR):
        running = target[row_at]
        for inner_at in range(row_at):
            running = running - factor[row_at, inner_at] * forward[inner_at]
        forward.append(running * inverse[row_at])
    result = [None] * PAR
    for row_at in reversed(range(PAR)):
        running = forward[row_at]
        for inner_at in range(row_at + 1, PAR):
            running = running - factor[inner_at, row_at] * result[inner_at]
        result[row_at] = running * inverse[row_at]
    return result


def two_parts(value):
    high = value.astype(bf16)
    low = (value - high.astype(f32)).astype(bf16)
    return jnp.concatenate([high, low], axis=0)


def joined(value):
    half = value.shape[0] // 2
    return value[:half] + value[half:]


def dot_nn(left, right):
    return lax.dot_general(left, right, (((1,), (0,)), ((), ())), preferred_element_type=f32)


def dot_nt(left, right):
    return lax.dot_general(left, right, (((1,), (1,)), ((), ())), preferred_element_type=f32)


def kernel(
    n_sky, n_tm,
    source_ref, knot_ref, count_ref, src_ref, att_ref, phase_ref, value_ref, prior_ref,
    sol_ref, res_ref, out_ref,
    hot_k, hot_s, rows_k, rows_s, y_ref, u0_ref, u1_ref,
    acc_a, acc_s, acc_k, taps_ref, z_ref,
    buf_a, buf_t, buf_f, buf_e,
    field_b, field_r, field_p, field_x,
    ss_t, rs_t, ss_f, rs_f, ss_e, rs_e,
):
    me_s = lax.axis_index("sky")
    me_t = lax.axis_index("tm")
    slots = source_ref.shape[1]
    hk = n_sky
    hs = prior_ref.shape[1] // LANES
    main = COMP * hk
    chunks = slots // CHUNK

    barrier = pltpu.get_barrier_semaphore()
    for ds in range(n_sky):
        for dt in range(n_tm):
            if ds or dt:
                pl.semaphore_signal(
                    barrier, inc=1,
                    device_id={"sky": lax.rem(me_s + ds, n_sky), "tm": lax.rem(me_t + dt, n_tm)},
                    device_id_type=pl.DeviceIdType.MESH,
                )

    def span(at):
        return pl.ds(pl.multiple_of(at * CHUNK, CHUNK), CHUNK)

    acc_a[...] = jnp.zeros_like(acc_a)

    def prepare(at, _):
        here = span(at)
        lane = lax.broadcasted_iota(jnp.int32, (1, CHUNK), 1) + at * CHUNK
        live = (lane < count_ref[0]).astype(f32)
        source = source_ref[:, here]
        src_low, src_high = source & (LANES - 1), source >> 7
        hot_s_here = (
            lax.broadcasted_iota(jnp.int32, (LANES, CHUNK), 0) == src_low
        ).astype(f32).astype(bf16)
        hot_s[:, here] = hot_s_here
        mask_s = (lax.broadcasted_iota(jnp.int32, (hs, CHUNK), 0) == src_high).astype(f32)
        observed = value_ref[:, here] * live
        y_ref[:, here] = observed
        designs = [src_ref[e : e + 1, here] * live for e in range(PAR)]
        masked = [mask_s * design for design in designs]
        for e in range(PAR):
            rows_s[e * hs : (e + 1) * hs, here] = masked[e]
        products = jnp.concatenate(
            [masked[i] * designs[j] for i, j in entry_pairs]
            + [masked[e] * observed for e in range(PAR)],
            axis=0,
        )
        acc_a[...] += dot_nt(two_parts(products), hot_s_here)
        return 0

    lax.fori_loop(0, chunks, prepare, 0)

    def prepare_knots(at, _):
        here = span(at)
        lane = lax.broadcasted_iota(jnp.int32, (1, CHUNK), 1) + at * CHUNK
        live = (lane < count_ref[0]).astype(f32)
        knot = knot_ref[:, here]
        knot_low, knot_high = knot & (KN_DEV - 1), knot >> 8
        hot_k[:, here] = (
            lax.broadcasted_iota(jnp.int32, (KN_DEV, CHUNK), 0) == knot_low
        ).astype(f32).astype(bf16)
        mask_k = (lax.broadcasted_iota(jnp.int32, (hk, CHUNK), 0) == knot_high).astype(f32)
        weights = spline_taps(phase_ref[:, here])
        for c in range(COMP):
            design = att_ref[c : c + 1, here] * live
            for m in range(TAPS):
                base = (c * TAPS + m) * hk
                rows_k[base : base + hk, here] = mask_k * (design * weights[m])
        return 0

    def over_tm(buf, stage):
        copies = []
        for d in range(1, n_tm):
            copy = pltpu.make_async_remote_copy(
                src_ref=buf.at[me_t], dst_ref=buf.at[me_t],
                send_sem=ss_t.at[stage, d - 1], recv_sem=rs_t.at[stage, d - 1],
                device_id={"sky": me_s, "tm": lax.rem(me_t + d, n_tm)},
                device_id_type=pl.DeviceIdType.MESH,
            )
            copy.start()
            copies.append(copy)
        return copies

    def finish(copies):
        for copy in copies:
            copy.wait()

    def edge_offsets(stage):
        return range(n_tm) if stage == 2 else sorted({0, 1, n_tm - 1})

    def over_sky(stage):
        mine = buf_f.at[stage, me_s]
        row = buf_e.at[stage, me_t, me_s]
        copies = []
        for ds in range(1, n_sky):
            copies.append(pltpu.make_async_remote_copy(
                src_ref=mine, dst_ref=mine,
                send_sem=ss_f.at[stage, ds - 1], recv_sem=rs_f.at[stage, ds - 1],
                device_id={"sky": lax.rem(me_s + ds, n_sky), "tm": me_t},
                device_id_type=pl.DeviceIdType.MESH,
            ))
        for dt in edge_offsets(stage):
            for ds in range(n_sky):
                if ds or dt:
                    copies.append(pltpu.make_async_remote_copy(
                        src_ref=row, dst_ref=row,
                        send_sem=ss_e.at[stage, dt, ds], recv_sem=rs_e.at[stage, dt, ds],
                        device_id={"sky": lax.rem(me_s + ds, n_sky), "tm": lax.rem(me_t + dt, n_tm)},
                        device_id_type=pl.DeviceIdType.MESH,
                    ))
        for copy in copies:
            copy.start()
        for copy in copies:
            copy.wait()

    def added(buf, count):
        total = buf[0]
        for at in range(1, count):
            total = total + buf[at]
        return total

    def elimination(v_of, stage):
        acc_k[...] = jnp.zeros_like(acc_k)

        def step(at, energy):
            here = span(at)
            picked = joined(dot_nn(z_ref[...], hot_s[:, here]))
            fitted = jnp.sum(rows_s[:, here] * picked, axis=0, keepdims=True)
            value = v_of(here)
            cleaned = value - fitted
            acc_k[...] += dot_nt(two_parts(rows_k[:, here] * cleaned), hot_k[:, here])
            return energy + value * cleaned

        energy = lax.fori_loop(0, chunks, step, jnp.zeros((1, CHUNK), f32))
        lane = lax.broadcasted_iota(jnp.int32, (hk, KN_DEV), 1)
        row = lax.broadcasted_iota(jnp.int32, (hk, KN_DEV), 0)
        pairs = TAPS * COMP * hk
        blocks, overs, firsts = [], [], []
        for c in range(COMP):
            block, over = None, None
            for m in range(TAPS):
                base = (c * TAPS + m) * hk
                part = acc_k[base : base + hk, :] + acc_k[pairs + base : pairs + base + hk, :]
                if m == 0:
                    block = part
                    continue
                turned = pltpu.roll(part, m, 1)
                above = pltpu.roll(turned, 1, 0)
                block = block + jnp.where(lane >= m, turned, jnp.where(row > 0, above, 0.0))
                past = jnp.where(lane[:1] < m, above[:1], 0.0)
                over = past if over is None else over + past
            blocks.append(block)
            overs.append(over)
            firsts.append(block[:1])
        buf_f[stage, me_s] = jnp.concatenate(blocks, axis=0)
        edge_lane = lax.broadcasted_iota(jnp.int32, (1, LANES), 1)
        packed = jnp.where(edge_lane == SCALAR, jnp.sum(energy, axis=1, keepdims=True), 0.0)
        for c in range(COMP):
            past = jnp.where(edge_lane < TAPS - 1, overs[c][:, :LANES], 0.0)
            first = jnp.where(edge_lane < TAPS - 1, firsts[c][:, :LANES], 0.0)
            packed = packed + (pltpu.roll(past, 8 * c, 1) if c else past) + pltpu.roll(first, 8 * (COMP + c), 1)
        buf_e[stage, me_t, me_s] = packed

    def knot_field(stage):
        total = added(buf_f.at[stage], n_sky)
        own = added(buf_e.at[stage, me_t], n_sky)
        before = added(buf_e.at[stage, lax.rem(me_t + n_tm - 1, n_tm)], n_sky)
        after = added(buf_e.at[stage, lax.rem(me_t + 1, n_tm)], n_sky)
        edge_lane = lax.broadcasted_iota(jnp.int32, (1, LANES), 1)
        rest = jnp.zeros((1, KN_DEV - LANES), f32)

        def unpacked(packed, at):
            turned = pltpu.roll(packed, LANES - 8 * at, 1) if at else packed
            return jnp.concatenate([jnp.where(edge_lane < TAPS - 1, turned, 0.0), rest], axis=1)

        lane = lax.broadcasted_iota(jnp.int32, (hk, KN_DEV), 1)
        row = lax.broadcasted_iota(jnp.int32, (hk, KN_DEV), 0)
        has_before = (me_t > 0).astype(f32)
        has_after = (me_t < n_tm - 1).astype(f32)
        corner = jnp.logical_and(lane < TAPS - 1, row == 0)
        blocks = []
        for c in range(COMP):
            block = total[c * hk : (c + 1) * hk]
            blocks.append(block + jnp.where(corner, unpacked(before, c) * has_before, 0.0))
        edge = jnp.concatenate(
            [(unpacked(own, c) + unpacked(after, COMP + c)) * has_after for c in range(COMP)], axis=0
        )
        return jnp.concatenate(blocks + [edge, jnp.zeros_like(edge)], axis=0)

    def along_knots(field, u_ref):
        lane = lax.broadcasted_iota(jnp.int32, (hk, KN_DEV), 1)
        row = lax.broadcasted_iota(jnp.int32, (hk, KN_DEV), 0)
        shifts = []
        for c in range(COMP):
            block = field[c * hk : (c + 1) * hk]
            below = jnp.where(row == hk - 1, field[main + c : main + c + 1], pltpu.roll(block, hk - 1, 0))
            shifts.append(block)
            for m in range(1, TAPS):
                shifts.append(pltpu.roll(jnp.where(lane < m, below, block), KN_DEV - m, 1))
        taps_ref[...] = two_parts(jnp.concatenate(shifts, axis=0))
        acc_s[...] = jnp.zeros_like(acc_s)

        def step(at, _):
            here = span(at)
            picked = joined(dot_nn(taps_ref[...], hot_k[:, here]))
            mapped = jnp.sum(rows_k[:, here] * picked, axis=0, keepdims=True)
            u_ref[:, here] = mapped
            acc_s[...] += dot_nt(two_parts(rows_s[:, here] * mapped), hot_s[:, here])
            return 0

        lax.fori_loop(0, chunks, step, 0)
        return joined(acc_s[...])

    def tiles(value):
        return [value[e * hs : (e + 1) * hs] for e in range(PAR)]

    def scalars(*values):
        row = lax.broadcasted_iota(jnp.int32, (8, LANES), 0)
        tile = jnp.zeros((8, LANES), f32)
        for at, value in enumerate(values):
            tile = jnp.where(row == at, value, tile)
        return tile

    def inner(left, right):
        return jnp.sum(left[:main] * right[:main])

    buf_a[me_t] = joined(acc_a[...])
    pl.semaphore_wait(barrier, n_sky * n_tm - 1)
    copies = over_tm(buf_a, 0)
    lax.fori_loop(0, chunks, prepare_knots, 0)
    finish(copies)
    sums = added(buf_a, n_tm)
    normal = {}
    for entry_at, pair in enumerate(entry_pairs):
        entry = sums[entry_at * hs : (entry_at + 1) * hs]
        if pair[0] == pair[1]:
            e = pair[0]
            entry = entry + jnp.concatenate(
                [prior_ref[e : e + 1, h * LANES : (h + 1) * LANES] for h in range(hs)], axis=0
            )
        normal[pair] = entry
    factor, inverse = factorize(normal)
    sums_y = sums[len(entry_pairs) * hs :]

    def solved(value):
        return chol_solve(factor, inverse, tiles(value))

    def solve_into_z(value):
        z_ref[...] = two_parts(jnp.concatenate(solved(value), axis=0))

    solve_into_z(sums_y)
    elimination(lambda here: y_ref[:, here], 0)
    over_sky(0)
    field_b[...] = knot_field(0)

    size = PAR * hs
    buf_t[0, me_t, :size, :] = along_knots(field_b[...], u0_ref)
    finish(over_tm(buf_t.at[0, :, pl.ds(0, size)], 1))
    sums_0 = added(buf_t.at[0, :, pl.ds(0, size)], n_tm)
    solve_into_z(sums_0)
    elimination(lambda here: u0_ref[:, here], 1)
    over_sky(1)
    b = field_b[...]
    q = knot_field(1) + damping * b
    field_x[...] = q

    buf_t[1, me_t, :size, :] = along_knots(q, u1_ref)
    buf_t[1, me_t, size:, :] = scalars(inner(b, b), inner(b, q), inner(q, q))
    finish(over_tm(buf_t.at[1], 2))
    total = added(buf_t.at[1], n_tm)
    norm_0, b_q, q_q = (total[size + at : size + at + 1, :1] for at in range(3))
    alpha_0 = norm_0 / b_q
    norm_1 = norm_0 - alpha_0 * (2.0 * b_q - alpha_0 * q_q)
    beta_0 = norm_1 / norm_0
    sums_1 = (1.0 + beta_0) * sums_0 - alpha_0 * total[:size]
    solve_into_z(sums_1)
    residual = field_b[...] - alpha_0 * field_x[...]
    field_r[...] = residual
    field_p[...] = residual + beta_0 * field_b[...]
    elimination(lambda here: (1.0 + beta_0) * u0_ref[:, here] - alpha_0 * u1_ref[:, here], 2)
    over_sky(2)
    direction = field_p[...]
    q = knot_field(2) + damping * direction
    residual = field_r[...]
    energy = added(buf_e.at[2, 0], n_sky)
    for t in range(1, n_tm):
        energy = energy + added(buf_e.at[2, t], n_sky)
    alpha_1 = norm_1 / (energy[:, SCALAR : SCALAR + 1] + damping * (1.0 + beta_0) * norm_1)
    field_x[...] = alpha_0 * field_b[...] + alpha_1 * direction
    field_r[...] = residual - alpha_1 * q
    for c in range(COMP):
        sol_ref[c] = field_x[pl.ds(c * hk + me_s, 1), :]
        res_ref[c] = field_r[pl.ds(c * hk + me_s, 1), :]
    last = solved(sums_y - alpha_0 * sums_0 - alpha_1 * sums_1)
    for e in range(PAR):
        for h in range(hs):
            out_ref[e : e + 1, h * LANES : (h + 1) * LANES] = last[e][h : h + 1]


def hand_over(*refs):
    for at in range(3):
        refs[3 + at][...] = refs[at][...]


def solution(mesh):
    n_sky, n_tm = mesh.shape["sky"], mesh.shape["tm"]

    def shards(obs_source, obs_knot, obs_count, src_design, att_design, obs_phase, obs_value, src_prior):
        slots = obs_source.shape[0]
        hk, hs = n_sky, src_prior.shape[1] // LANES
        pairs = COMP * TAPS * hk
        main = COMP * hk
        entries = len(entry_pairs) + PAR
        vmem = pl.BlockSpec(memory_space=pltpu.VMEM)
        smem = pl.BlockSpec(memory_space=pltpu.SMEM)
        dma = pltpu.SemaphoreType.DMA
        results = pl.pallas_call(
            functools.partial(kernel, n_sky, n_tm),
            out_shape=(
                jax.ShapeDtypeStruct((COMP, 1, KN_DEV), f32),
                jax.ShapeDtypeStruct((COMP, 1, KN_DEV), f32),
                jax.ShapeDtypeStruct(src_prior.shape, f32),
            ),
            in_specs=[vmem, vmem, smem, vmem, vmem, vmem, vmem, vmem],
            out_specs=(vmem, vmem, vmem),
            scratch_shapes=[
                pltpu.VMEM((KN_DEV, slots), bf16),
                pltpu.VMEM((LANES, slots), bf16),
                pltpu.VMEM((pairs, slots), f32),
                pltpu.VMEM((PAR * hs, slots), f32),
                pltpu.VMEM((1, slots), f32),
                pltpu.VMEM((1, slots), f32),
                pltpu.VMEM((1, slots), f32),
                pltpu.VMEM((2 * entries * hs, LANES), f32),
                pltpu.VMEM((2 * PAR * hs, LANES), f32),
                pltpu.VMEM((2 * pairs, KN_DEV), f32),
                pltpu.VMEM((2 * pairs, KN_DEV), bf16),
                pltpu.VMEM((2 * PAR * hs, LANES), bf16),
                pltpu.VMEM((n_tm, entries * hs, LANES), f32),
                pltpu.VMEM((2, n_tm, PAR * hs + 8, LANES), f32),
                pltpu.VMEM((3, n_sky, main, KN_DEV), f32),
                pltpu.VMEM((3, n_tm, n_sky, 1, LANES), f32),
                pltpu.VMEM((main + 8, KN_DEV), f32),
                pltpu.VMEM((main + 8, KN_DEV), f32),
                pltpu.VMEM((main + 8, KN_DEV), f32),
                pltpu.VMEM((main + 8, KN_DEV), f32),
                dma((3, n_tm - 1)), dma((3, n_tm - 1)),
                dma((3, n_sky - 1)), dma((3, n_sky - 1)),
                dma((3, n_tm, n_sky)), dma((3, n_tm, n_sky)),
            ],
            compiler_params=pltpu.CompilerParams(collective_id=0, has_side_effects=True),
        )(
            obs_source.reshape(1, slots), obs_knot.reshape(1, slots), obs_count,
            src_design, att_design, obs_phase.reshape(1, slots), obs_value.reshape(1, slots), src_prior,
        )
        return pl.pallas_call(
            hand_over,
            out_shape=tuple(jax.ShapeDtypeStruct(result.shape, f32) for result in results),
            in_specs=[vmem] * 3,
            out_specs=(vmem,) * 3,
        )(*results)

    placed = (
        P(("sky", "tm")),
        P(("sky", "tm")),
        P(("sky", "tm")),
        P(None, ("sky", "tm")),
        P(None, ("sky", "tm")),
        P(("sky", "tm")),
        P(("sky", "tm")),
        P(None, "sky"),
    )
    return jax.shard_map(
        shards,
        mesh=mesh,
        in_specs=placed,
        out_specs=(P(None, "tm", "sky"), P(None, "tm", "sky"), P(None, "sky")),
        check_vma=False,
    )
```
